32 devices in a mesh: row: 8 (over z, core), col: 4 (over y, x).
Axes of the slice: x: 2, y: 2, z: 4, core: 2. Of those that a mesh axis runs over, the one named last changes fastest.
Arguments:
- matrix: bfloat16 [4096, 4096], P('row', 'col'), may hold values from -6 to 6
- factors: float32 [4096, 4096], P('row', 'col')
- inverse: bfloat16 [32, 128, 128], P('col'), may hold values from -0.007171631 to 0.007171631
- pattern: int32 [32, 32], P('row', 'col'), may hold values from 0 to 1, as said below
- dropped: int32 [32, 32], P('row', 'col'), may hold values from 0 to 1, as said below
Outputs:
- factors_out: float32 [4096, 4096], P('row', 'col')
The draws below stay inside these ranges and needn't reach their ends.
Inputs may be any that keep to these rules, and one draw needn't show every extreme that they name: Block (I, J) can be in the pattern only where I - J is 0, 1, -1, 4, -4, 16 or -16; the blocks with I - J of 0, 1, -1, 4 and -4 are always in it. In each device's region of 4 block rows by 8 block columns, every block column holds at most 3 pattern blocks (exactly 3 in some columns), and every block row at most 2 pattern blocks below the block diagonal (exactly 2 in some rows). `dropped`: dropped blocks lie in the pattern and off the block diagonal.
All inputs are finite; a program needn't handle non-finite values.
Results may differ from the reference program's by a relative error of at most 0.00083.
Values may be sent and summed in bfloat16 or wider, within the bound.
A program may use at most 128 MiB of HBM per device.

```python
import jax
import jax.numpy as jnp
from jax import lax

BS = 128
RB = 4
SWEEPS = 2
NB = 32
N = 4096


def pattern_from(key):
    row_number = jnp.arange(NB)[:, None]
    col_number = jnp.arange(NB)[None, :]
    offset = jnp.abs(row_number - col_number)
    band = (offset <= 1) | (offset == RB)
    far = offset == NB // 2
    lowest = jnp.minimum(row_number, col_number)
    coin_vector = jax.random.randint(jax.random.fold_in(key, 11), (NB,), 0, 2)
    keep_far = (coin_vector[lowest] == 1) | (lowest % RB == 0)
    return (band | far & keep_far).astype(jnp.int32)


def draw_pattern(key, part):
    return pattern_from(key)


def draw_dropped(key, part):
    member = pattern_from(key)
    coin = jax.random.randint(jax.random.fold_in(key, 13), (NB, NB), 0, 4) == 0
    row_number = jnp.arange(NB)[:, None]
    col_number = jnp.arange(NB)[None, :]
    off_diagonal = row_number != col_number
    return (member * coin * off_diagonal).astype(jnp.int32)


def draw_factors(key, part):
    block_number = jnp.arange(N) // BS
    below = block_number[:, None] > block_number[None, :]
    spread = jnp.where(below, 0.015, 1.0).astype(jnp.float32)
    raw_values = jax.random.normal(key, (N, N), jnp.float32)
    return (raw_values * spread).astype(jnp.float32)


def block_levels(rng, extent, split, smallest, high):
    factor_of, own = 1.0, jax.random.fold_in(rng, 6)
    for axis_at, blocks in split:
        steps = jnp.exp(jax.random.uniform(jax.random.fold_in(own, axis_at), (blocks,), jnp.float32, smallest / len(split), high / len(split)))
        factor_of = factor_of * jnp.repeat(steps, extent[axis_at] // blocks).reshape([-1 if axis == axis_at else 1 for axis in range(len(extent))])
    return factor_of


def normal_values(own_key, extent, width, bound, split=(), kind=jnp.bfloat16):
    level = block_levels(own_key, extent, split, -0.22, 0.18) if split else 1.0
    entries = jax.random.normal(own_key, extent, jnp.float32) * width * level
    return jnp.minimum(jnp.maximum(entries, -bound), bound).astype(kind)


def setup_inputs(seed: int = 0) -> dict:
    streams_of = jax.random.split(jax.random.key(seed), 6)
    matrix = normal_values(streams_of[0], (N, N), 1.0, 6.0, ((0, 8), (1, 4)))
    factors = draw_factors(jax.random.fold_in(streams_of[5], 71), 0)
    inverse = normal_values(streams_of[2], (NB, BS, BS), 0.0012, 0.007171631, ((0, 4),))
    pattern = draw_pattern(jax.random.fold_in(streams_of[5], 71), 0)
    dropped = draw_dropped(jax.random.fold_in(streams_of[5], 71), 0)
    return {"matrix": matrix, "factors": factors, "inverse": inverse, "pattern": pattern, "dropped": dropped}


def expand(block_mask):
    return jnp.repeat(jnp.repeat(block_mask, BS, axis=0), BS, axis=1)


def reference(matrix, factors, inverse, pattern, dropped):
    row_number = jnp.arange(NB)[:, None]
    col_number = jnp.arange(NB)[None, :]
    member = pattern == 1
    lower_mask = expand((member & (row_number > col_number)).astype(jnp.float32))
    upper_mask = expand((member & (row_number <= col_number)).astype(jnp.float32))
    in_pattern = expand(member.astype(jnp.float32))
    low_part = factors * lower_mask
    up_part = factors * upper_mask
    dense_matrix = matrix.astype(jnp.float32)
    inverse_full = inverse.astype(jnp.float32)
    for sweep_index in range(SWEEPS):
        low_half = lax.optimization_barrier(low_part.astype(jnp.bfloat16)).astype(jnp.float32)
        up_half = lax.optimization_barrier(up_part.astype(jnp.bfloat16)).astype(jnp.float32)
        product = jnp.dot(low_half, up_half, precision=lax.Precision.HIGHEST)
        residual = (dense_matrix - product - up_part) * in_pattern
        rounded = lax.optimization_barrier(residual.astype(jnp.bfloat16)).astype(jnp.float32)
        rounded = rounded.reshape(N, NB, BS)
        correction = jnp.einsum("rjb,jbc->rjc", rounded, inverse_full, precision=lax.Precision.HIGHEST)
        low_part = low_part + correction.reshape(N, N) * lower_mask
        up_part = up_part + residual * upper_mask
    keep_mask = expand((1 - dropped).astype(jnp.float32))
    return (low_part + up_part) * keep_mask
```

```python
import functools

import jax
import jax.numpy as jnp
from jax import lax
from jax.experimental import pallas as pl
from jax.experimental.pallas import tpu as pltpu
from jax.sharding import PartitionSpec as P

SWEEPS = 2
MESH = pl.DeviceIdType.MESH
F32 = jnp.float32
BF16 = jnp.bfloat16

SLOTS = 4
DIAG, LEFT, RIGHT, OUTER = range(SLOTS)
D_NEAR, D_FAR, L_NEAR, U_NEAR, L_FAR, U_FAR = range(6)


def dot(x, y):
    return jnp.dot(x, y, preferred_element_type=F32)


def sweep_kernel(
    rows, cols, row_devices, col_devices, bs,
    pattern, dropped, matrix, factors, inverse_in, out,
    a, inverse, lb, ub, sd, rd, rln, run, rlf, ruf, acc,
    load_sem, inverse_sem, send_sem, recv_sem,
):
    r, c = lax.axis_index("row"), lax.axis_index("col")
    far_r, far_c = row_devices // 2, col_devices // 2
    q = r - (cols // rows) * c
    barrier = pltpu.get_barrier_semaphore()

    def loads(i, s, j):
        k = i * SLOTS + s
        src = (pl.ds(i * bs, bs), pl.ds(pl.multiple_of(j * bs, bs), bs))
        return (
            pltpu.make_async_copy(factors.at[src], out.at[k], load_sem.at[0, k]),
            pltpu.make_async_copy(matrix.at[src], a.at[k], load_sem.at[1, k]),
        )

    def start_loads(blocks):
        for block in blocks:
            for copy in loads(*block):
                copy.start()

    def wait_loads(blocks):
        for block in blocks:
            for copy in loads(*block):
                copy.wait()

    inverse_copy = pltpu.make_async_copy(inverse_in, inverse, inverse_sem)

    def hello(r2, c2):
        pl.semaphore_signal(barrier, inc=1, device_id=(r2, c2), device_id_type=MESH)

    def message(kind, v, src, dst, slot, r2, c2):
        return pltpu.make_async_remote_copy(
            src_ref=src, dst_ref=dst,
            send_sem=send_sem.at[kind, v], recv_sem=recv_sem.at[slot, v],
            device_id=(r2, c2), device_id_type=MESH,
        )

    def d_near(v):
        return message(D_NEAR, v, sd.at[v], rd.at[v], D_NEAR, r + 1, c)

    def d_far(v):
        return message(D_FAR, v, sd.at[v], rd.at[v], D_NEAR, r + far_r, c)

    def l_near(v):
        return message(L_NEAR, v, lb.at[v, pl.ds(0, rows + 1)], rln.at[v], L_NEAR, r, c + 1)

    def u_near(v):
        return message(U_NEAR, v, ub.at[v, pl.ds(0, rows + 1)], run.at[v], U_NEAR, r + 1, c)

    def l_far(v):
        return message(L_FAR, v, lb.at[v, pl.ds(0, rows)], rlf.at[v], L_FAR, r, c + far_c)

    def u_far(v):
        return message(U_FAR, v, ub.at[v, pl.ds(0, rows)], ruf.at[v], U_FAR, r + far_r, c)

    def lower_step(k, b, v, diag, j, mask=None):
        product = dot(lb[v, b], diag)
        residual = a[k].astype(F32) - product
        if mask is not None:
            residual = residual * mask
        correction = dot(residual.astype(BF16), inverse[j])
        if mask is not None:
            correction = correction * mask
        out[k] = out[k] + correction
        if v + 1 < SWEEPS:
            lb[v + 1, b] = out[k].astype(BF16)

    def upper_steps(k, b, mask=None):
        for v in range(SWEEPS):
            ub[v, b] = out[k].astype(BF16)
            residual = a[k].astype(F32) - out[k]
            if mask is not None:
                residual = residual * mask
            out[k] = out[k] + residual

    def keep(i, s, j):
        k = i * SLOTS + s
        out[k] = out[k] * (1 - dropped[i, j]).astype(F32)

    out[rows * SLOTS] = jnp.zeros((bs, bs), F32)

    def diagonal_owner(h):
        base = h * rows
        below = [(i, LEFT, base + i - 1) for i in range(rows) if base + i >= 1]
        right = [(i, RIGHT, base + i + 1) for i in range(rows) if base + i + 1 < cols]
        diag = [(i, DIAG, base + i) for i in range(rows)]
        outer = [(i, OUTER, i if h else rows + i) for i in range(rows)]
        has_far = c >= far_c
        sends_far = c < far_c
        has_near = c >= 1
        sends_near = c + 1 < col_devices

        def when_near_in(f):
            if h:
                f()
            else:
                pl.when(has_near)(f)

        def when_near_out(f):
            if h:
                pl.when(sends_near)(f)
            else:
                f()

        start_loads(diag)
        start_loads(outer)
        start_loads(right)
        start_loads(below)
        inverse_copy.start()

        def hello_near():
            hello(r - 1, c)
            if not h:
                hello(r, c - 1)

        when_near_in(hello_near)

        @pl.when(has_far)
        def _():
            hello(r - far_r, c)
            hello(r, c - far_c)

        wait_loads(diag)
        for i in range(rows):
            sd[0, i] = out[i * SLOTS + DIAG].astype(BF16)
        near_peers = sends_near.astype(jnp.int32) if h else 1
        peers = near_peers + sends_far.astype(jnp.int32)
        pl.when(peers > 0)(lambda: pl.semaphore_wait(barrier, peers))

        def send_d(v):
            pl.when(sends_far)(lambda: d_far(v).start())
            when_near_out(lambda: d_near(v).start())

        send_d(0)
        wait_loads(outer)
        wait_loads(right)
        for i, s, j in right:
            upper_steps(i * SLOTS + s, 2 * rows - 1 - i)
        if not h:
            for i, s, j in outer:
                upper_steps(i * SLOTS + s, i)
            u_near(0).start()
            u_near(1).start()
        wait_loads(below)
        for i, s, j in below:
            lb[0, rows + i] = out[i * SLOTS + s].astype(BF16)
        if h:
            for i, s, j in outer:
                lb[0, i] = out[i * SLOTS + s].astype(BF16)
        inverse_copy.wait()

        for v in range(SWEEPS):
            acc[0] = jnp.zeros((bs, bs), F32)
            for i in range(1, rows):
                acc[i] = dot(lb[v, rows + i], ub[v, 2 * rows - i])

            def near_terms():
                u_near_in = message(U_NEAR, v, ub.at[v, pl.ds(0, rows + 1)], run.at[v], U_NEAR, r - 1, c)
                u_near_in.wait_recv()
                if h:
                    left = lb
                else:
                    message(L_NEAR, v, lb.at[v, pl.ds(0, rows + 1)], rln.at[v], L_NEAR, r, c - 1).wait_recv()
                    left = rln
                acc[0] = acc[0] + dot(left[v, rows], run[v, rows])
                for i in range(rows):
                    acc[i] = acc[i] + dot(left[v, i], run[v, i])

            def far_terms():
                message(U_FAR, v, ub.at[v, pl.ds(0, rows)], ruf.at[v], U_FAR, r - far_r, c).wait_recv()
                message(L_FAR, v, lb.at[v, pl.ds(0, rows)], rlf.at[v], L_FAR, r, c - far_c).wait_recv()
                for i in range(rows):
                    acc[i] = acc[i] + dot(rlf[v, i], ruf[v, i])

            def local_lower():
                for i in range(1, rows):
                    lower_step(i * SLOTS + LEFT, rows + i, v, sd[v, i - 1], base + i - 1)

            def lower_from_before():
                if h:
                    message(D_NEAR, v, sd.at[v], rd.at[v], D_NEAR, r - 1, c).wait_recv()
                    lower_step(LEFT, rows, v, rd[v, rows - 1], rows - 1)
                    for i in range(rows):
                        lower_step(i * SLOTS + OUTER, i, v, rd[v, i], i)

            def diag_step():
                for i in range(rows):
                    k = i * SLOTS + DIAG
                    residual = a[k].astype(F32) - acc[i] - out[k]
                    out[k] = out[k] + residual
                    if v + 1 < SWEEPS:
                        sd[v + 1, i] = out[k].astype(BF16)
                if v + 1 < SWEEPS:
                    send_d(v + 1)

            local_lower()
            when_near_in(near_terms)
            if v + 1 < SWEEPS:
                pl.when(has_far)(far_terms)
                diag_step()
                lower_from_before()
            else:
                lower_from_before()
                pl.when(has_far)(far_terms)
                diag_step()

        for i, s, j in below + right + outer:
            keep(i, s, j)
        for v in range(SWEEPS):
            when_near_out(lambda: d_near(v).wait_send())
            pl.when(sends_far)(lambda: d_far(v).wait_send())
            if not h:
                u_near(v).wait_send()

    def lower_owner(blocks, source_r, l_message, far):
        places = [(i, s, j) for i, s, j, b, n in blocks]
        start_loads(places)
        inverse_copy.start()
        hello(source_r, c)
        wait_loads(places)
        masks = {}
        for i, s, j, b, n in blocks:
            k = i * SLOTS + s
            masks[k] = pattern[i, j].astype(F32) if far else None
            if far:
                out[k] = out[k] * masks[k]
            lb[0, b] = out[k].astype(BF16)
        pl.semaphore_wait(barrier, 1)
        l_message(0).start()
        inverse_copy.wait()
        for v in range(SWEEPS):
            message(D_NEAR, v, sd.at[v], rd.at[v], D_NEAR, source_r, c).wait_recv()
            for i, s, j, b, n in blocks:
                k = i * SLOTS + s
                lower_step(k, b, v, rd[v, n], j, masks[k])
            if v + 1 < SWEEPS:
                l_message(v + 1).start()
        for i, s, j in places:
            keep(i, s, j)
        for v in range(SWEEPS):
            l_message(v).wait_send()

    def upper_owner(blocks, u_message, far):
        places = [(i, s, j) for i, s, j, b in blocks]
        start_loads(places)
        wait_loads(places)
        for i, s, j, b in blocks:
            k = i * SLOTS + s
            mask = pattern[i, j].astype(F32) if far else None
            if far:
                out[k] = out[k] * mask
            upper_steps(k, b, mask)
        pl.semaphore_wait(barrier, 1)
        for v in range(SWEEPS):
            u_message(v).start()
        for i, s, j in places:
            keep(i, s, j)
        for v in range(SWEEPS):
            u_message(v).wait_send()

    pl.when(q == 0)(lambda: diagonal_owner(0))
    pl.when(q == 1)(lambda: diagonal_owner(1))

    @pl.when(q == 2)
    def _():
        blocks = [(i, OUTER, rows + i, i, i) for i in range(rows)]
        lower_owner(blocks + [(0, LEFT, cols - 1, rows, rows - 1)], r - 1, l_near, False)

    @pl.when(q == -1)
    def _():
        blocks = [(i, OUTER, i, i) for i in range(rows)]
        upper_owner(blocks + [(rows - 1, RIGHT, 0, rows)], u_near, False)

    @pl.when((q == far_r) | (q == far_r + 1))
    def _():
        base = (q - far_r) * rows
        blocks = [(i, OUTER, base + i, i, i) for i in range(rows)]
        lower_owner(blocks, r - far_r, l_far, True)

    @pl.when((q == -far_r) | (q == 1 - far_r))
    def _():
        base = (q + far_r) * rows
        blocks = [(i, OUTER, base + i, i) for i in range(rows)]
        upper_owner(blocks, u_far, True)


def place_kernel(rows, cols, row_devices, bs, blocks, out, sem):
    r, c = lax.axis_index("row"), lax.axis_index("col")
    q = r - (cols // rows) * c
    far = (row_devices // 2) * rows
    copies = []
    for i in range(rows):
        for j in range(cols):
            d = rows * q + i - j
            k = jnp.where(
                d == 0, i * SLOTS + DIAG,
                jnp.where(
                    d == 1, i * SLOTS + LEFT,
                    jnp.where(
                        d == -1, i * SLOTS + RIGHT,
                        jnp.where(
                            (d == rows) | (d == -rows) | (d == far) | (d == -far),
                            i * SLOTS + OUTER, rows * SLOTS,
                        ),
                    ),
                ),
            )
            dst = out.at[pl.ds(i * bs, bs), pl.ds(j * bs, bs)]
            copies.append(pltpu.make_async_copy(blocks.at[k], dst, sem.at[i * cols + j]))
    for copy in copies:
        copy.start()
    for copy in copies:
        copy.wait()


def solution(mesh):
    row_devices, col_devices = mesh.shape["row"], mesh.shape["col"]

    def on_device(matrix, factors, inverse, pattern, dropped):
        rows, cols = pattern.shape
        bs = inverse.shape[1]
        places = rows * SLOTS
        half = lambda *n: pltpu.VMEM(n + (bs, bs), BF16)
        hbm = pl.BlockSpec(memory_space=pl.ANY)
        smem = pl.BlockSpec(memory_space=pltpu.SMEM)
        vmem = pl.BlockSpec(memory_space=pltpu.VMEM)
        blocks = pl.pallas_call(
            functools.partial(sweep_kernel, rows, cols, row_devices, col_devices, bs),
            out_shape=jax.ShapeDtypeStruct((places + 1, bs, bs), F32),
            in_specs=[smem, smem, hbm, hbm, hbm],
            out_specs=vmem,
            scratch_shapes=[
                half(places), half(cols), half(SWEEPS, 2 * rows), half(SWEEPS, 2 * rows),
                half(SWEEPS, rows), half(SWEEPS, rows),
                half(SWEEPS, rows + 1), half(SWEEPS, rows + 1), half(SWEEPS, rows), half(SWEEPS, rows),
                pltpu.VMEM((rows, bs, bs), F32),
                pltpu.SemaphoreType.DMA((2, places)),
                pltpu.SemaphoreType.DMA,
                pltpu.SemaphoreType.DMA((6, SWEEPS)),
                pltpu.SemaphoreType.DMA((6, SWEEPS)),
            ],
            compiler_params=pltpu.CompilerParams(collective_id=0, has_side_effects=True),
            name="sweeps",
        )(pattern, dropped, matrix, factors, inverse)
        return pl.pallas_call(
            functools.partial(place_kernel, rows, cols, row_devices, bs),
            out_shape=jax.ShapeDtypeStruct(factors.shape, F32),
            in_specs=[vmem],
            out_specs=hbm,
            scratch_shapes=[pltpu.SemaphoreType.DMA((rows * cols,))],
            name="place",
        )(blocks)

    placed = (P("row", "col"), P("row", "col"), P("col", None, None), P("row", "col"), P("row", "col"))
    return jax.shard_map(
        on_device, mesh=mesh, in_specs=placed, out_specs=P("row", "col"), check_vma=False
    )
```

```python
import functools

import jax
import jax.numpy as jnp
from jax import lax
from jax.experimental import pallas as pl
from jax.experimental.pallas import tpu as pltpu
from jax.sharding import PartitionSpec as P

SWEEPS = 2
MESH = pl.DeviceIdType.MESH
F32 = jnp.float32
BF16 = jnp.bfloat16

SLOTS = 4
DIAG, LEFT, RIGHT, OUTER = range(SLOTS)
D_NEAR, D_FAR, L_NEAR, U_NEAR, L_FAR, U_FAR = range(6)


def dot(x, y):
    return jnp.dot(x, y, preferred_element_type=F32)


def sweep_kernel(
    rows, cols, row_devices, col_devices, bs,
    pattern, dropped, matrix, factors, inverse_in, out,
    a, inverse, lb, ub, ua, sd, rd, rln, run, rlf, ruf, acc,
    load_sem, inverse_sem, send_sem, recv_sem,
):
    r, c = lax.axis_index("row"), lax.axis_index("col")
    far_r, far_c = row_devices // 2, col_devices // 2
    q = r - (cols // rows) * c
    barrier = pltpu.get_barrier_semaphore()

    def loads(i, s, j):
        k = s * rows + i
        src = (pl.ds(i * bs, bs), pl.ds(pl.multiple_of(j * bs, bs), bs))
        return (
            pltpu.make_async_copy(factors.at[src], out.at[k], load_sem.at[0, k]),
            pltpu.make_async_copy(matrix.at[src], a.at[k], load_sem.at[1, k]),
        )

    def start_loads(blocks):
        for block in blocks:
            for copy in loads(*block):
                copy.start()

    def wait_loads(blocks):
        for block in blocks:
            for copy in loads(*block):
                copy.wait()

    inverse_copy = pltpu.make_async_copy(inverse_in, inverse, inverse_sem)

    def hello(r2, c2):
        pl.semaphore_signal(barrier, inc=1, device_id=(r2, c2), device_id_type=MESH)

    def message(kind, v, b, src, dst, slot, r2, c2):
        return pltpu.make_async_remote_copy(
            src_ref=src, dst_ref=dst.at[v, b],
            send_sem=send_sem.at[kind, v, b], recv_sem=recv_sem.at[slot, v, b],
            device_id=(r2, c2), device_id_type=MESH,
        )

    def receive(slot, v, b, dst, r2, c2):
        message(slot, v, b, dst.at[v, b], dst, slot, r2, c2).wait_recv()

    def d_near(v, b):
        return message(D_NEAR, v, b, sd.at[v, b], rd, D_NEAR, r + 1, c)

    def d_far(v, b):
        return message(D_FAR, v, b, sd.at[v, b], rd, D_NEAR, r + far_r, c)

    def l_near(v, b):
        return message(L_NEAR, v, b, lb.at[v, b], rln, L_NEAR, r, c + 1)

    def l_far(v, b):
        return message(L_FAR, v, b, lb.at[v, b], rlf, L_FAR, r, c + far_c)

    def u_near(v, b):
        k = OUTER * rows + b if b < rows else RIGHT * rows + rows - 1
        src = a.at[k] if v else ub.at[b]
        return message(U_NEAR, v, b, src, run, U_NEAR, r + 1, c)

    def u_far(v, b):
        src = ua.at[b] if v else ub.at[b]
        return message(U_FAR, v, b, src, ruf, U_FAR, r + far_r, c)

    def kept(i, j):
        return (1 - dropped[i, j]).astype(F32)

    def lower_step(i, s, j, b, v, diag, mask=None):
        k = s * rows + i
        residual = a[k].astype(F32) - dot(lb[v, b], diag)
        if mask is not None:
            residual = residual * mask
        correction = dot(residual.astype(BF16), inverse[j])
        if mask is not None:
            correction = correction * mask
        new = out[k] + correction
        if v + 1 < SWEEPS:
            out[k] = new
            lb[v + 1, b] = new.astype(BF16)
        else:
            out[k] = new * kept(i, j)

    out[rows * SLOTS] = jnp.zeros((bs, bs), F32)

    def diagonal_owner(h):
        base = h * rows
        below = [(i, LEFT, base + i - 1) for i in range(rows) if base + i >= 1]
        right = [(i, RIGHT, base + i + 1) for i in range(rows) if base + i + 1 < cols]
        diag = [(i, DIAG, base + i) for i in range(rows)]
        outer = [(i, OUTER, i if h else rows + i) for i in range(rows)]
        has_far = c >= far_c
        sends_far = c < far_c
        has_near = c >= 1
        sends_near = c + 1 < col_devices

        def when_near_in(f):
            if h:
                f()
            else:
                pl.when(has_near)(f)

        def when_near_out(f):
            if h:
                pl.when(sends_near)(f)
            else:
                f()

        start_loads(diag)
        start_loads(outer)
        start_loads(right)
        start_loads(below)
        inverse_copy.start()

        def hello_near():
            hello(r - 1, c)
            if not h:
                hello(r, c - 1)

        when_near_in(hello_near)

        @pl.when(has_far)
        def _():
            hello(r - far_r, c)
            hello(r, c - far_c)

        wait_loads(diag)
        for i in range(rows):
            sd[0, i] = out[DIAG * rows + i].astype(BF16)
        near_peers = sends_near.astype(jnp.int32) if h else 1
        peers = near_peers + sends_far.astype(jnp.int32)
        pl.when(peers > 0)(lambda: pl.semaphore_wait(barrier, peers))

        @pl.when(sends_far)
        def _():
            for b in range(rows):
                d_far(0, b).start()

        def send_first_near():
            for b in range(rows):
                d_near(0, b).start()

        when_near_out(send_first_near)
        wait_loads(outer)
        wait_loads(right)
        for i, s, j in right:
            ub[2 * rows - 1 - i] = out[s * rows + i].astype(BF16)
        if not h:
            for i, s, j in outer:
                ub[i] = out[s * rows + i].astype(BF16)
            for v in range(SWEEPS):
                for b in range(rows + 1):
                    u_near(v, b).start()
        for i, s, j in right + ([] if h else outer):
            out[s * rows + i] = a[s * rows + i].astype(F32) * kept(i, j)
        wait_loads(below)
        for i, s, j in below:
            lb[0, rows + i] = out[s * rows + i].astype(BF16)
        if h:
            for i, s, j in outer:
                lb[0, i] = out[s * rows + i].astype(BF16)
        inverse_copy.wait()

        def lower_blocks(v):
            for i in range(1, rows):
                lower_step(i, LEFT, base + i - 1, rows + i, v, sd[v, i - 1])
            if h:
                for i in range(rows):
                    receive(D_NEAR, v, i, rd, r - 1, c)
                    lower_step(i, OUTER, i, i, v, rd[v, i])
                lower_step(0, LEFT, rows - 1, rows, v, rd[v, rows - 1])

        def diag_blocks(v):
            acc[0] = jnp.zeros((bs, bs), F32)
            for i in range(1, rows):
                u = a[RIGHT * rows + i - 1] if v else ub[2 * rows - i]
                acc[i] = dot(lb[v, rows + i], u)

            def near_terms():
                left = lb if h else rln
                for b in list(range(rows)) + [rows]:
                    receive(U_NEAR, v, b, run, r - 1, c)
                    if not h:
                        receive(L_NEAR, v, b, rln, r, c - 1)
                    i = b % rows
                    acc[i] = acc[i] + dot(left[v, b], run[v, b])

            when_near_in(near_terms)

            def finish(i, product):
                k = DIAG * rows + i
                new = a[k].astype(F32) - product
                if v + 1 < SWEEPS:
                    sd[v + 1, i] = new.astype(BF16)
                else:
                    out[k] = new * kept(i, base + i)

            @pl.when(has_far)
            def _():
                for i in range(rows):
                    receive(U_FAR, v, i, ruf, r - far_r, c)
                    receive(L_FAR, v, i, rlf, r, c - far_c)
                    finish(i, acc[i] + dot(rlf[v, i], ruf[v, i]))

            @pl.when(sends_far)
            def _():
                for i in range(rows):
                    finish(i, acc[i])
                if v + 1 < SWEEPS:
                    for i in range(rows):
                        d_far(v + 1, i).start()

            if v + 1 < SWEEPS:

                def send_near():
                    for i in range(rows):
                        d_near(v + 1, i).start()

                when_near_out(send_near)

        diag_blocks(0)
        for v in range(SWEEPS):
            lower_blocks(v)
        diag_blocks(1)

        def near_sent():
            for v in range(SWEEPS):
                for b in range(rows):
                    d_near(v, b).wait_send()

        when_near_out(near_sent)

        @pl.when(sends_far)
        def _():
            for v in range(SWEEPS):
                for b in range(rows):
                    d_far(v, b).wait_send()

        if not h:
            for v in range(SWEEPS):
                for b in range(rows + 1):
                    u_near(v, b).wait_send()

    def lower_owner(blocks, source_r, l_message, far):
        places = [(i, s, j) for i, s, j, b, n in blocks]
        start_loads(places)
        inverse_copy.start()
        hello(source_r, c)
        wait_loads(places)
        masks = {}
        for i, s, j, b, n in blocks:
            k = s * rows + i
            masks[k] = pattern[i, j].astype(F32) if far else None
            if far:
                out[k] = out[k] * masks[k]
            lb[0, b] = out[k].astype(BF16)
        pl.semaphore_wait(barrier, 1)
        for i, s, j, b, n in blocks:
            l_message(0, b).start()
        inverse_copy.wait()
        for v in range(SWEEPS):
            for i, s, j, b, n in blocks:
                if b == n:
                    receive(D_NEAR, v, n, rd, source_r, c)
                lower_step(i, s, j, b, v, rd[v, n], masks[s * rows + i])
                if v + 1 < SWEEPS:
                    l_message(v + 1, b).start()
        for v in range(SWEEPS):
            for i, s, j, b, n in blocks:
                l_message(v, b).wait_send()

    def upper_owner(blocks, u_message, far):
        places = [(i, s, j) for i, s, j, b in blocks]
        start_loads(places)
        wait_loads(places)
        for i, s, j, b in blocks:
            k = s * rows + i
            if far:
                mask = pattern[i, j].astype(F32)
                ub[b] = (out[k] * mask).astype(BF16)
                masked = a[k].astype(F32) * mask
                ua[b] = masked.astype(BF16)
                out[k] = masked * kept(i, j)
            else:
                ub[b] = out[k].astype(BF16)
                out[k] = a[k].astype(F32) * kept(i, j)
        pl.semaphore_wait(barrier, 1)
        for v in range(SWEEPS):
            for i, s, j, b in blocks:
                u_message(v, b).start()
        for v in range(SWEEPS):
            for i, s, j, b in blocks:
                u_message(v, b).wait_send()

    pl.when(q == 0)(lambda: diagonal_owner(0))
    pl.when(q == 1)(lambda: diagonal_owner(1))

    @pl.when(q == 2)
    def _():
        blocks = [(i, OUTER, rows + i, i, i) for i in range(rows)]
        lower_owner(blocks + [(0, LEFT, cols - 1, rows, rows - 1)], r - 1, l_near, False)

    @pl.when(q == -1)
    def _():
        blocks = [(i, OUTER, i, i) for i in range(rows)]
        upper_owner(blocks + [(rows - 1, RIGHT, 0, rows)], u_near, False)

    @pl.when((q == far_r) | (q == far_r + 1))
    def _():
        base = (q - far_r) * rows
        blocks = [(i, OUTER, base + i, i, i) for i in range(rows)]
        lower_owner(blocks, r - far_r, l_far, True)

    @pl.when((q == -far_r) | (q == 1 - far_r))
    def _():
        base = (q + far_r) * rows
        blocks = [(i, OUTER, base + i, i) for i in range(rows)]
        upper_owner(blocks, u_far, True)


def place_kernel(rows, cols, row_devices, bs, blocks, out, sem):
    r, c = lax.axis_index("row"), lax.axis_index("col")
    q = r - (cols // rows) * c
    far = (row_devices // 2) * rows
    copies = []
    for i in range(rows):
        for j in range(cols):
            d = rows * q + i - j
            k = jnp.where(
                d == 0, DIAG * rows + i,
                jnp.where(
                    d == 1, LEFT * rows + i,
                    jnp.where(
                        d == -1, RIGHT * rows + i,
                        jnp.where(
                            (d == rows) | (d == -rows) | (d == far) | (d == -far),
                            OUTER * rows + i, rows * SLOTS,
                        ),
                    ),
                ),
            )
            dst = out.at[pl.ds(i * bs, bs), pl.ds(j * bs, bs)]
            copies.append(pltpu.make_async_copy(blocks.at[k], dst, sem.at[i * cols + j]))
    for copy in copies:
        copy.start()
    for copy in copies:
        copy.wait()


def solution(mesh):
    row_devices, col_devices = mesh.shape["row"], mesh.shape["col"]

    def on_device(matrix, factors, inverse, pattern, dropped):
        rows, cols = pattern.shape
        bs = inverse.shape[1]
        places = rows * SLOTS
        half = lambda *n: pltpu.VMEM(n + (bs, bs), BF16)
        hbm = pl.BlockSpec(memory_space=pltpu.HBM)
        smem = pl.BlockSpec(memory_space=pltpu.SMEM)
        vmem = pl.BlockSpec(memory_space=pltpu.VMEM)
        blocks = pl.pallas_call(
            functools.partial(sweep_kernel, rows, cols, row_devices, col_devices, bs),
            out_shape=jax.ShapeDtypeStruct((places + 1, bs, bs), F32),
            in_specs=[smem, smem, hbm, hbm, hbm],
            out_specs=vmem,
            scratch_shapes=[
                half(places), half(cols), half(SWEEPS, 2 * rows), half(2 * rows), half(rows),
                half(SWEEPS, rows), half(SWEEPS, rows),
                half(SWEEPS, rows + 1), half(SWEEPS, rows + 1), half(SWEEPS, rows), half(SWEEPS, rows),
                pltpu.VMEM((rows, bs, bs), F32),
                pltpu.SemaphoreType.DMA((2, places)),
                pltpu.SemaphoreType.DMA,
                pltpu.SemaphoreType.DMA((6, SWEEPS, rows + 1)),
                pltpu.SemaphoreType.DMA((6, SWEEPS, rows + 1)),
            ],
            compiler_params=pltpu.CompilerParams(collective_id=0, has_side_effects=True),
            name="sweeps",
        )(pattern, dropped, matrix, factors, inverse)
        return pl.pallas_call(
            functools.partial(place_kernel, rows, cols, row_devices, bs),
            out_shape=jax.ShapeDtypeStruct(factors.shape, F32),
            in_specs=[vmem],
            out_specs=hbm,
            scratch_shapes=[pltpu.SemaphoreType.DMA((rows * cols,))],
            name="place",
        )(blocks)

    placed = (P("row", "col"), P("row", "col"), P("col", None, None), P("row", "col"), P("row", "col"))
    return jax.shard_map(
        on_device, mesh=mesh, in_specs=placed, out_specs=P("row", "col"), check_vma=False
    )
```

```python
import functools

import jax
import jax.numpy as jnp
from jax import lax
from jax.experimental import pallas as pl
from jax.experimental.pallas import tpu as pltpu
from jax.sharding import PartitionSpec as P

SWEEPS = 2
MESH = pl.DeviceIdType.MESH
F32 = jnp.float32
BF16 = jnp.bfloat16

SLOTS = 4
DIAG, LEFT, RIGHT, OUTER = range(SLOTS)
D_NEAR, D_FAR, L_NEAR, U_NEAR, L_FAR, U_FAR = range(6)


def dot(x, y):
    return jnp.dot(x, y, preferred_element_type=F32)


def sweep_kernel(
    rows, cols, row_devices, col_devices, bs,
    pattern, dropped, matrix, factors, inverse_in, out,
    a, inverse, lb, ub, ua, sd, rd, rln, run, rlf, ruf, acc,
    load_sem, inverse_sem, send_sem, recv_sem,
):
    r, c = lax.axis_index("row"), lax.axis_index("col")
    far_r, far_c = row_devices // 2, col_devices // 2
    q = r - (cols // rows) * c
    barrier = pltpu.get_barrier_semaphore()

    def loads(i, s, j):
        k = s * rows + i
        src = (pl.ds(i * bs, bs), pl.ds(pl.multiple_of(j * bs, bs), bs))
        return (
            pltpu.make_async_copy(factors.at[src], out.at[k], load_sem.at[0, k]),
            pltpu.make_async_copy(matrix.at[src], a.at[k], load_sem.at[1, k]),
        )

    def start_loads(blocks):
        for block in blocks:
            for copy in loads(*block):
                copy.start()

    def wait_loads(blocks):
        for block in blocks:
            for copy in loads(*block):
                copy.wait()

    inverse_copy = pltpu.make_async_copy(inverse_in, inverse, inverse_sem)

    def hello(r2, c2):
        pl.semaphore_signal(barrier, inc=1, device_id=(r2, c2), device_id_type=MESH)

    def message(kind, v, src, dst, slot, r2, c2):
        return pltpu.make_async_remote_copy(
            src_ref=src, dst_ref=dst.at[v],
            send_sem=send_sem.at[kind, v], recv_sem=recv_sem.at[slot, v],
            device_id=(r2, c2), device_id_type=MESH,
        )

    def receive(slot, v, dst, r2, c2):
        message(slot, v, dst.at[v], dst, slot, r2, c2).wait_recv()

    def d_near(v):
        return message(D_NEAR, v, sd.at[v], rd, D_NEAR, r + 1, c)

    def d_far(v):
        return message(D_FAR, v, sd.at[v], rd, D_NEAR, r + far_r, c)

    def l_near(v):
        return message(L_NEAR, v, lb.at[v, pl.ds(0, rows + 1)], rln, L_NEAR, r, c + 1)

    def l_far(v):
        return message(L_FAR, v, lb.at[v, pl.ds(0, rows)], rlf, L_FAR, r, c + far_c)

    def u_near(v):
        src = a.at[pl.ds(OUTER * rows - 1, rows + 1)] if v else ub.at[pl.ds(0, rows + 1)]
        return message(U_NEAR, v, src, run, U_NEAR, r + 1, c)

    def u_far(v):
        src = ua if v else ub.at[pl.ds(1, rows)]
        return message(U_FAR, v, src, ruf, U_FAR, r + far_r, c)

    def kept(i, j):
        return (1 - dropped[i, j]).astype(F32)

    def lower_step(i, s, j, b, v, diag, mask=None):
        k = s * rows + i
        residual = a[k].astype(F32) - dot(lb[v, b], diag)
        if mask is not None:
            residual = residual * mask
        correction = dot(residual.astype(BF16), inverse[j])
        if mask is not None:
            correction = correction * mask
        new = out[k] + correction
        if v + 1 < SWEEPS:
            out[k] = new
            lb[v + 1, b] = new.astype(BF16)
        else:
            out[k] = new * kept(i, j)

    def diagonal_owner(h):
        base = h * rows
        below = [(i, LEFT, base + i - 1) for i in range(rows) if base + i >= 1]
        right = [(i, RIGHT, base + i + 1) for i in range(rows) if base + i + 1 < cols]
        diag = [(i, DIAG, base + i) for i in range(rows)]
        outer = [(i, OUTER, i if h else rows + i) for i in range(rows)]
        has_far = c >= far_c
        sends_far = c < far_c
        has_near = c >= 1
        sends_near = c + 1 < col_devices

        def when_near_in(f):
            if h:
                f()
            else:
                pl.when(has_near)(f)

        def when_near_out(f):
            if h:
                pl.when(sends_near)(f)
            else:
                f()

        start_loads(diag)
        start_loads(outer)
        start_loads(right)
        start_loads(below)
        inverse_copy.start()

        def hello_near():
            hello(r - 1, c)
            if not h:
                hello(r, c - 1)

        when_near_in(hello_near)

        @pl.when(has_far)
        def _():
            hello(r - far_r, c)
            hello(r, c - far_c)

        wait_loads(diag)
        for i in range(rows):
            sd[0, i] = out[DIAG * rows + i].astype(BF16)
        near_peers = sends_near.astype(jnp.int32) if h else 1
        peers = near_peers + sends_far.astype(jnp.int32)
        pl.when(peers > 0)(lambda: pl.semaphore_wait(barrier, peers))

        @pl.when(sends_far)
        def _():
            d_far(0).start()

        def send_first_near():
            d_near(0).start()

        when_near_out(send_first_near)
        wait_loads(outer)
        wait_loads(right)
        for i, s, j in right:
            ub[0 if i == rows - 1 else rows + 1 + i] = out[s * rows + i].astype(BF16)
        if not h:
            for i, s, j in outer:
                ub[1 + i] = out[s * rows + i].astype(BF16)
            for v in range(SWEEPS):
                u_near(v).start()
        for i, s, j in right + ([] if h else outer):
            out[s * rows + i] = a[s * rows + i].astype(F32) * kept(i, j)
        wait_loads(below)
        for i, s, j in below:
            lb[0, rows + i] = out[s * rows + i].astype(BF16)
        if h:
            for i, s, j in outer:
                lb[0, i] = out[s * rows + i].astype(BF16)
        inverse_copy.wait()

        def lower_blocks(v):
            for i in range(1, rows):
                lower_step(i, LEFT, base + i - 1, rows + i, v, sd[v, i - 1])
            if h:
                receive(D_NEAR, v, rd, r - 1, c)
                for i in range(rows):
                    lower_step(i, OUTER, i, i, v, rd[v, i])
                lower_step(0, LEFT, rows - 1, rows, v, rd[v, rows - 1])

        def diag_blocks(v):
            acc[0] = jnp.zeros((bs, bs), F32)
            for i in range(1, rows):
                u = a[RIGHT * rows + i - 1] if v else ub[rows + i]
                acc[i] = dot(lb[v, rows + i], u)

            def near_terms():
                left = lb if h else rln
                receive(U_NEAR, v, run, r - 1, c)
                if not h:
                    receive(L_NEAR, v, rln, r, c - 1)
                acc[0] = acc[0] + dot(left[v, rows], run[v, 0])
                for i in range(rows):
                    acc[i] = acc[i] + dot(left[v, i], run[v, 1 + i])

            when_near_in(near_terms)

            def finish(i, product):
                k = DIAG * rows + i
                new = a[k].astype(F32) - product
                if v + 1 < SWEEPS:
                    sd[v + 1, i] = new.astype(BF16)
                else:
                    out[k] = new * kept(i, base + i)

            @pl.when(has_far)
            def _():
                receive(U_FAR, v, ruf, r - far_r, c)
                receive(L_FAR, v, rlf, r, c - far_c)
                for i in range(rows):
                    finish(i, acc[i] + dot(rlf[v, i], ruf[v, i]))

            @pl.when(sends_far)
            def _():
                for i in range(rows):
                    finish(i, acc[i])
                if v + 1 < SWEEPS:
                    d_far(v + 1).start()

            if v + 1 < SWEEPS:
                when_near_out(lambda: d_near(v + 1).start())

        diag_blocks(0)
        for v in range(SWEEPS):
            lower_blocks(v)
        diag_blocks(1)

        def near_sent():
            for v in range(SWEEPS):
                d_near(v).wait_send()

        when_near_out(near_sent)

        @pl.when(sends_far)
        def _():
            for v in range(SWEEPS):
                d_far(v).wait_send()

        if not h:
            for v in range(SWEEPS):
                u_near(v).wait_send()

    def lower_owner(blocks, source_r, l_message, far):
        places = [(i, s, j) for i, s, j, b, n in blocks]
        start_loads(places)
        inverse_copy.start()
        hello(source_r, c)
        wait_loads(places)
        masks = {}
        for i, s, j, b, n in blocks:
            k = s * rows + i
            masks[k] = pattern[i, j].astype(F32) if far else None
            if far:
                out[k] = out[k] * masks[k]
            lb[0, b] = out[k].astype(BF16)
        pl.semaphore_wait(barrier, 1)
        l_message(0).start()
        inverse_copy.wait()
        for v in range(SWEEPS):
            receive(D_NEAR, v, rd, source_r, c)
            for i, s, j, b, n in blocks:
                lower_step(i, s, j, b, v, rd[v, n], masks[s * rows + i])
            if v + 1 < SWEEPS:
                l_message(v + 1).start()
        for v in range(SWEEPS):
            l_message(v).wait_send()

    def upper_owner(blocks, u_message, far):
        places = [(i, s, j) for i, s, j, b in blocks]
        start_loads(places)
        wait_loads(places)
        for i, s, j, b in blocks:
            k = s * rows + i
            if far:
                mask = pattern[i, j].astype(F32)
                ub[b] = (out[k] * mask).astype(BF16)
                masked = a[k].astype(F32) * mask
                ua[b - 1] = masked.astype(BF16)
                out[k] = masked * kept(i, j)
            else:
                ub[b] = out[k].astype(BF16)
                out[k] = a[k].astype(F32) * kept(i, j)
        pl.semaphore_wait(barrier, 1)
        for v in range(SWEEPS):
            u_message(v).start()
        for v in range(SWEEPS):
            u_message(v).wait_send()

    pl.when(q == 0)(lambda: diagonal_owner(0))
    pl.when(q == 1)(lambda: diagonal_owner(1))

    @pl.when(q == 2)
    def _():
        blocks = [(i, OUTER, rows + i, i, i) for i in range(rows)]
        lower_owner(blocks + [(0, LEFT, cols - 1, rows, rows - 1)], r - 1, l_near, False)

    @pl.when(q == -1)
    def _():
        blocks = [(i, OUTER, i, 1 + i) for i in range(rows)]
        upper_owner(blocks + [(rows - 1, RIGHT, 0, 0)], u_near, False)

    @pl.when((q == far_r) | (q == far_r + 1))
    def _():
        base = (q - far_r) * rows
        blocks = [(i, OUTER, base + i, i, i) for i in range(rows)]
        lower_owner(blocks, r - far_r, l_far, True)

    @pl.when((q == -far_r) | (q == 1 - far_r))
    def _():
        base = (q + far_r) * rows
        blocks = [(i, OUTER, base + i, 1 + i) for i in range(rows)]
        upper_owner(blocks, u_far, True)


def place_kernel(rows, cols, row_devices, bs, blocks, out, held, zero, load_sem, sem):
    r, c = lax.axis_index("row"), lax.axis_index("col")
    q = r - (cols // rows) * c
    far = (row_devices // 2) * rows
    load = pltpu.make_async_copy(blocks, held, load_sem)
    load.start()
    zero[...] = jnp.zeros_like(zero)
    places = []
    for i in range(rows):
        for j in range(cols):
            d = rows * q + i - j
            outer = (d == rows) | (d == -rows) | (d == far) | (d == -far)
            near = (d == 0) | (d == 1) | (d == -1)
            slot = jnp.where(
                d == 0, DIAG, jnp.where(d == 1, LEFT, jnp.where(d == -1, RIGHT, OUTER))
            )
            dst = out.at[pl.ds(i * bs, bs), pl.ds(j * bs, bs)]
            places.append((outer | near, slot * rows + i, dst, sem.at[i * cols + j]))
    for kept, k, dst, done in places:
        pl.when(~kept)(lambda: pltpu.make_async_copy(zero, dst, done).start())
    load.wait()
    for kept, k, dst, done in places:
        pl.when(kept)(lambda: pltpu.make_async_copy(held.at[k], dst, done).start())
    for kept, k, dst, done in places:
        pltpu.make_async_copy(zero, dst, done).wait()


def solution(mesh):
    row_devices, col_devices = mesh.shape["row"], mesh.shape["col"]

    def on_device(matrix, factors, inverse, pattern, dropped):
        rows, cols = pattern.shape
        bs = inverse.shape[1]
        places = rows * SLOTS
        half = lambda *n: pltpu.VMEM(n + (bs, bs), BF16)
        hbm = pl.BlockSpec(memory_space=pltpu.HBM)
        smem = pl.BlockSpec(memory_space=pltpu.SMEM)
        vmem = pl.BlockSpec(memory_space=pltpu.VMEM)
        blocks = pl.pallas_call(
            functools.partial(sweep_kernel, rows, cols, row_devices, col_devices, bs),
            out_shape=jax.ShapeDtypeStruct((places, bs, bs), F32),
            in_specs=[smem, smem, hbm, hbm, hbm],
            out_specs=vmem,
            scratch_shapes=[
                half(places), half(cols), half(SWEEPS, 2 * rows), half(2 * rows), half(rows),
                half(SWEEPS, rows), half(SWEEPS, rows),
                half(SWEEPS, rows + 1), half(SWEEPS, rows + 1), half(SWEEPS, rows), half(SWEEPS, rows),
                pltpu.VMEM((rows, bs, bs), F32),
                pltpu.SemaphoreType.DMA((2, places)),
                pltpu.SemaphoreType.DMA,
                pltpu.SemaphoreType.DMA((6, SWEEPS)),
                pltpu.SemaphoreType.DMA((6, SWEEPS)),
            ],
            compiler_params=pltpu.CompilerParams(collective_id=0, has_side_effects=True),
            name="sweeps",
        )(pattern, dropped, matrix, factors, inverse)
        return pl.pallas_call(
            functools.partial(place_kernel, rows, cols, row_devices, bs),
            out_shape=jax.ShapeDtypeStruct(factors.shape, F32),
            in_specs=[hbm],
            out_specs=hbm,
            scratch_shapes=[
                pltpu.VMEM((places, bs, bs), F32),
                pltpu.VMEM((bs, bs), F32),
                pltpu.SemaphoreType.DMA,
                pltpu.SemaphoreType.DMA((rows * cols,)),
            ],
            name="place",
        )(blocks)

    placed = (P("row", "col"), P("row", "col"), P("col", None, None), P("row", "col"), P("row", "col"))
    return jax.shard_map(
        on_device, mesh=mesh, in_specs=placed, out_specs=P("row", "col"), check_vma=False
    )
```
